32 devices in a mesh: gx: 8 (over y, x, core), gy: 4 (over z).
Axes of the slice: x: 2, y: 2, z: 4, core: 2. Of those that a mesh axis runs over, the one named last changes fastest.
Arguments:
- pair_in: bfloat16 [256, 256, 128], P(('gx', 'gy')), may hold values from -6 to 6
- residue_mask: int32 [256], P(('gx', 'gy')), may hold values 0 or 1
- norm_start: float32 [128], replicated, may hold values from 0.25 to 1.75
- proj_start: bfloat16 [128, 512], replicated, may hold values from -0.5 to 0.5
- gate_bias_start: float32 [128], replicated, may hold values from -4 to 4
- bias_w_start: bfloat16 [128, 4], replicated, may hold values from -1.5 to 1.5
- out_w_start: bfloat16 [128, 128], replicated, may hold values from -1 to 1
- norm_end: float32 [128], replicated, may hold values from 0.25 to 1.75
- proj_end: bfloat16 [128, 512], replicated, may hold values from -0.5 to 0.5
- gate_bias_end: float32 [128], replicated, may hold values from -4 to 4
- bias_w_end: bfloat16 [128, 4], replicated, may hold values from -1.5 to 1.5
- out_w_end: bfloat16 [128, 128], replicated, may hold values from -1 to 1
- norm_trans: float32 [128], replicated, may hold values from 0.25 to 1.75
- trans_in: bfloat16 [128, 512], replicated, may hold values from -0.5 to 0.5
- trans_bias: float32 [512], replicated, may hold values from -4 to 4
- trans_out: bfloat16 [512, 128], replicated, may hold values from -0.375 to 0.375
Outputs:
- pair_out: bfloat16 [256, 256, 128], P(('gx', 'gy'))
The draws below stay inside these ranges and needn't reach their ends.
Inputs may be any that keep to these rules, and one draw needn't show every extreme that they name: residue_mask holds only 0 and 1.
All inputs are finite; a program needn't handle non-finite values.
Results may differ from the reference program's by a relative error of at most 0.02.
Values may be sent and summed in bfloat16 or wider, within the bound.
A program may use at most 192 MiB of HBM per device.

```python
import jax
import jax.numpy as jnp
from jax import lax

C = 128
HEADS = 4
HEAD_DIM = 32
FFN = 512
RES = 256


def with_ends(array, key, smallest, top_value):
    place = [jax.random.randint(jax.random.fold_in(key, axis), (), 0, length) for axis, length in enumerate(array.shape)]
    longest = array.shape.index(max(array.shape))
    next_to = place[:longest] + [(place[longest] + 1) % array.shape[longest]] + place[longest + 1:]
    return array.at[tuple(place)].set(smallest).at[tuple(next_to)].set(top_value)


def block_scale(own_key, shape, split, least, high):
    loudness = 1.0
    for position, shards_of in split:
        steps = jax.random.uniform(jax.random.fold_in(jax.random.fold_in(own_key, 6), position), (shards_of,), jnp.float32, least / len(split), high / len(split))
        loudness = loudness * jnp.repeat(jnp.exp(steps), shape[position] // shards_of).reshape((-1,) + (1,) * (len(shape) - 1 - position))
    return loudness


def scatter_about(own_key, extent, deviation, bound, pieces=(), held_as=jnp.bfloat16):
    values = jax.random.normal(own_key, extent, jnp.float32) * deviation
    if len(pieces) > 0:
        values = block_scale(own_key, extent, pieces, -0.22, 0.18) * values
    return jnp.clip(values, min=-bound, max=bound).astype(held_as)


def setup_inputs(seed: int = 0) -> dict:
    streams_of = jax.random.split(jax.random.key(seed), 17)
    return {
        "pair_in": scatter_about(streams_of[0], (RES, RES, C), 1.0, 6.0, ((0, 32),)),
        "residue_mask": with_ends((jax.random.randint(streams_of[1], (RES,), 0, 8) < 7).astype(jnp.int32), jax.random.fold_in(streams_of[1], 1), 0, 1),
        "norm_start": jnp.clip(1.0 + 0.15 * jax.random.normal(streams_of[2], (C,), jnp.float32), 0.25, 1.75),
        "proj_start": scatter_about(streams_of[3], (C, 4 * C), C ** -0.5, 0.5),
        "gate_bias_start": scatter_about(streams_of[4], (C,), 1.0, 4.0, (), jnp.float32),
        "bias_w_start": scatter_about(streams_of[5], (C, HEADS), (C // 8) ** -0.5, 1.5),
        "out_w_start": scatter_about(streams_of[6], (C, C), (C // 4) ** -0.5, 1.0),
        "norm_end": jnp.clip(1.0 + 0.15 * jax.random.normal(streams_of[7], (C,), jnp.float32), 0.25, 1.75),
        "proj_end": scatter_about(streams_of[8], (C, 4 * C), C ** -0.5, 0.5),
        "gate_bias_end": scatter_about(streams_of[9], (C,), 1.0, 4.0, (), jnp.float32),
        "bias_w_end": scatter_about(streams_of[10], (C, HEADS), (C // 8) ** -0.5, 1.5),
        "out_w_end": scatter_about(streams_of[11], (C, C), (C // 4) ** -0.5, 1.0),
        "norm_trans": jnp.clip(1.0 + 0.15 * jax.random.normal(streams_of[12], (C,), jnp.float32), 0.25, 1.75),
        "trans_in": scatter_about(streams_of[13], (C, FFN), C ** -0.5, 0.5),
        "trans_bias": scatter_about(streams_of[14], (FFN,), 1.0, 4.0, (), jnp.float32),
        "trans_out": scatter_about(streams_of[15], (FFN, C), (FFN // 2) ** -0.5, 0.375),
    }


big_negative = 1000000000.0

def layer_norm(values, norm_gain):
    widened = values.astype(jnp.float32)
    row_mean = lax.optimization_barrier(jnp.mean(widened, axis=-1, keepdims=True))
    row_var = lax.optimization_barrier(jnp.mean(jnp.square(widened - row_mean), axis=-1, keepdims=True))
    return ((widened - row_mean) * lax.rsqrt(row_var + 1e-05) * norm_gain).astype(jnp.bfloat16)

def project(normed, weight):
    flat = normed.reshape(-1, normed.shape[-1])
    result = jnp.dot(flat, weight, preferred_element_type=jnp.float32)
    return result.reshape(normed.shape[:-1] + (weight.shape[1],))

def split_heads(merged):
    return merged.astype(jnp.bfloat16).reshape(merged.shape[:-1] + (HEADS, HEAD_DIM))

def attend_block(query, keys, values, pair_bias, key_bias):
    score_scale = HEAD_DIM ** (-0.5)
    scores = jnp.einsum('jhd,khd->hjk', query.astype(jnp.float32), keys.astype(jnp.float32), precision=lax.Precision.HIGHEST)
    scores = scores * score_scale + pair_bias + key_bias
    attn_weights = jax.nn.softmax(scores, axis=-1)
    mixed = jnp.einsum('hjk,khd->jhd', attn_weights, values.astype(jnp.float32), precision=lax.Precision.HIGHEST)
    return mixed.reshape(query.shape[0], HEADS * HEAD_DIM)

def gated_residual(residual, mixed, gate_logit, gate_bias, out_weight):
    gated = (mixed * jax.nn.sigmoid(gate_logit + gate_bias)).astype(jnp.bfloat16)
    return (residual.astype(jnp.float32) + project(gated, out_weight)).astype(jnp.bfloat16)

def projections(normed, weight, channels):
    projected = project(normed, weight)
    query = split_heads(projected[..., :channels])
    keys = split_heads(projected[..., channels:2 * channels])
    values = split_heads(projected[..., 2 * channels:3 * channels])
    return (query, keys, values, projected[..., 3 * channels:])

def reference(pair_in, residue_mask, norm_start, proj_start, gate_bias_start, bias_w_start, out_w_start, norm_end, proj_end, gate_bias_end, bias_w_end, out_w_end, norm_trans, trans_in, trans_bias, trans_out):
    channels = pair_in.shape[-1]
    key_bias = (residue_mask.astype(jnp.float32) - 1.0) * big_negative
    normed = layer_norm(pair_in, norm_start)
    query, keys, values, gate_logit = projections(normed, proj_start, channels)
    pair_bias = project(normed, bias_w_start).astype(jnp.bfloat16)
    start_bias = jnp.transpose(pair_bias, (2, 0, 1)).astype(jnp.float32)

    def per_row(operands):
        query_row, key_row, value_row = operands
        return attend_block(query_row, key_row, value_row, start_bias, key_bias)
    mixed = lax.map(per_row, (query, keys, values))
    after_start = gated_residual(pair_in, mixed, gate_logit, gate_bias_start, out_w_start)
    normed = layer_norm(after_start, norm_end)
    query, keys, values, gate_logit = projections(normed, proj_end, channels)
    pair_bias = project(normed, bias_w_end).astype(jnp.bfloat16)
    end_bias = jnp.transpose(pair_bias, (2, 1, 0)).astype(jnp.float32)

    def per_column(operands):
        query_col, key_col, value_col = operands
        return attend_block(query_col, key_col, value_col, end_bias, key_bias)
    mixed = lax.map(per_column, (jnp.swapaxes(query, 0, 1), jnp.swapaxes(keys, 0, 1), jnp.swapaxes(values, 0, 1)))
    mixed = jnp.swapaxes(mixed, 0, 1)
    after_end = gated_residual(after_start, mixed, gate_logit, gate_bias_end, out_w_end)
    normed = layer_norm(after_end, norm_trans)
    hidden = jax.nn.relu(project(normed, trans_in) + trans_bias).astype(jnp.bfloat16)
    return (after_end.astype(jnp.float32) + project(hidden, trans_out)).astype(jnp.bfloat16)
```

```python
import functools
import math

import jax
import jax.numpy as jnp
from jax import lax
from jax.experimental import pallas as pl
from jax.experimental.pallas import tpu as pltpu
from jax.sharding import PartitionSpec as P

HEADS = 4
HEAD_DIM = 32
BIG = 1000000000.0
LOG2E = math.log2(math.e)
QSCALE = HEAD_DIM ** (-0.5) * LOG2E
MESH = pl.DeviceIdType.MESH
F32 = jnp.float32
BF16 = jnp.bfloat16


def nn(a, b):
    return lax.dot_general(a, b, (((1,), (0,)), ((), ())), preferred_element_type=F32)


def nt(a, b):
    return lax.dot_general(a, b, (((1,), (1,)), ((), ())), preferred_element_type=F32)


def layer_norm(x, gain):
    mean = jnp.mean(x, axis=-1, keepdims=True)
    cent = x - mean
    var = jnp.mean(cent * cent, axis=-1, keepdims=True)
    return (cent * lax.rsqrt(var + 1e-05) * gain).astype(BF16)


def bias_rows(w, r, rows, normed):
    shape = (HEADS * rows, HEADS)
    place = lax.broadcasted_iota(jnp.int32, shape, 0) == (
        lax.broadcasted_iota(jnp.int32, shape, 1) * rows + r
    )
    spread = nt(place.astype(F32).astype(BF16), w).astype(BF16)
    return nt(spread, normed)


def head_mask(shape, h):
    lane = lax.broadcasted_iota(jnp.int32, shape, 1)
    return (lane >= h * HEAD_DIM) & (lane < (h + 1) * HEAD_DIM)


def attend(q, k, v, bias_ref, start, size):
    channels = q.shape[1]
    total = None
    for h in range(HEADS):
        mask = head_mask(k.shape, h)
        zero = jnp.zeros_like(k)
        scores = nt(q, jnp.where(mask, k, zero)) + bias_ref[h, pl.ds(start, size), :]
        top = jnp.max(scores, axis=-1, keepdims=True)
        weights = jnp.exp2(scores - top).astype(BF16)
        side = jnp.concatenate(
            [jnp.where(mask, v, zero), jnp.where(mask, jnp.ones_like(v), zero)], axis=1
        )
        part = nn(weights, side)
        total = part if total is None else total + part
    return total[:, :channels] / total[:, channels:]


def kernel(
    nx,
    ny,
    tq,
    x_ref,
    mask_ref,
    g1_ref,
    w1_ref,
    gb1_ref,
    bw1_ref,
    ow1_ref,
    g2_ref,
    w2_ref,
    gb2_ref,
    bw2_ref,
    ow2_ref,
    g3_ref,
    ti_ref,
    tb_ref,
    to_ref,
    out_ref,
    a_ref,
    q_ref,
    k_ref,
    v_ref,
    bias_ref,
    kb_ref,
    zs_ref,
    send_m,
    recv_m,
    send_a,
    recv_a,
    send_b,
    recv_b,
    send_z,
    recv_z,
    recv_o,
    ssem,
    rsem,
):
    n = nx * ny
    rows, res, ch = x_ref.shape
    me = lax.axis_index("gx") * ny + lax.axis_index("gy")

    def peer_of(t):
        return lax.rem(me + t, n)

    def coords(p):
        return (p // ny, lax.rem(p, ny))

    barrier = pltpu.get_barrier_semaphore()

    @pl.loop(1, n)
    def _(t):
        pl.semaphore_signal(barrier, inc=1, device_id=coords(peer_of(t)), device_id_type=MESH)

    def share(kind, src, dst, p):
        return pltpu.make_async_remote_copy(
            src_ref=src,
            dst_ref=dst.at[me],
            send_sem=ssem.at[kind, p],
            recv_sem=rsem.at[kind, me],
            device_id=coords(p),
            device_id_type=MESH,
        )

    def arrived(kind, src, dst, p):
        return pltpu.make_async_remote_copy(
            src_ref=src,
            dst_ref=dst.at[p],
            send_sem=ssem.at[kind, p],
            recv_sem=rsem.at[kind, p],
            device_id=coords(p),
            device_id_type=MESH,
        )

    def norm_row(r, acc):
        normed = layer_norm(x_ref[r].astype(F32), g1_ref[...])
        a_ref[r] = normed
        return acc + bias_rows(bw1_ref[...], r, rows, normed)

    acc = lax.fori_loop(0, rows, norm_row, jnp.zeros((HEADS * rows, res), F32))
    send_a[...] = acc.astype(BF16)
    lane = lax.broadcasted_iota(jnp.int32, (8, 128), 0) * 128 + lax.broadcasted_iota(
        jnp.int32, (8, 128), 1
    )
    vec = jnp.zeros((8, 128), F32)
    for t in range(rows):
        vec = jnp.where(lane == me * rows + t, mask_ref[t].astype(F32), vec)
    send_m[...] = vec

    pl.semaphore_wait(barrier, n - 1)

    @pl.loop(1, n)
    def _(t):
        p = peer_of(t)
        share(0, send_m, recv_m, p).start()
        share(1, send_a, recv_a, p).start()

    recv_m[me] = send_m[...]
    recv_a[me] = send_a[...]

    def project_row(r, carry):
        p = nn(a_ref[r], w1_ref[:, : 3 * ch])
        q_ref[r] = (p[:, :ch] * QSCALE).astype(BF16)
        k_ref[r] = p[:, ch : 2 * ch].astype(BF16)
        v_ref[r] = p[:, 2 * ch :].astype(BF16)
        return carry

    lax.fori_loop(0, rows, project_row, 0)

    @pl.loop(1, n)
    def _(t):
        p = peer_of(t)
        arrived(0, send_m, recv_m, p).wait()
        arrived(1, send_a, recv_a, p).wait()

    masks = jnp.sum(recv_m[...], axis=0)
    key_mask = jnp.concatenate([masks[t : t + 1, :] for t in range(res // 128)], axis=1)
    kb_ref[...] = (key_mask - 1.0) * BIG

    def start_bias(d, carry):
        block = (recv_a[d].astype(F32) + kb_ref[...]) * LOG2E
        for h in range(HEADS):
            bias_ref[h, pl.ds(pl.multiple_of(d * rows, rows), rows), :] = block[
                h * rows : (h + 1) * rows
            ]
        return carry

    lax.fori_loop(0, n, start_bias, 0)

    def start_row(r, acc):
        pieces = []
        for c in range(res // tq):
            lo = c * tq
            o = attend(q_ref[r, lo : lo + tq, :], k_ref[r], v_ref[r], bias_ref, lo, tq)
            gl = nn(a_ref[r, lo : lo + tq, :], w1_ref[:, 3 * ch :])
            gated = (o * jax.nn.sigmoid(gl + gb1_ref[...])).astype(BF16)
            z1 = x_ref[r, lo : lo + tq, :].astype(F32) + nn(gated, ow1_ref[...])
            z1 = z1.astype(BF16).astype(F32)
            zs_ref[lo // rows : (lo + tq) // rows, pl.ds(r, rows, stride=rows), :] = z1.reshape(
                tq // rows, rows, ch
            )
            pieces.append(layer_norm(z1, g2_ref[...]))
        normed = pieces[0] if len(pieces) == 1 else jnp.concatenate(pieces, axis=0)
        return acc + bias_rows(bw2_ref[...], r, rows, normed)

    acc = lax.fori_loop(0, rows, start_row, jnp.zeros((HEADS * rows, res), F32))
    send_b[...] = acc.astype(BF16)
    send_z[...] = zs_ref[...].astype(BF16)

    @pl.loop(1, n)
    def _(t):
        p = peer_of(t)
        share(2, send_b, recv_b, p).start()
        share(3, send_z.at[p], recv_z, p).start()

    recv_b[me] = send_b[...]
    recv_z[me] = send_z[me]

    @pl.loop(1, n)
    def _(t):
        p = peer_of(t)
        arrived(2, send_b, recv_b, p).wait()
        arrived(3, send_z.at[p], recv_z, p).wait()

    zs_ref[...] = recv_z[...].astype(F32)
    kd = 128 // rows
    for t in range(res // 128):
        block = recv_b[t * kd : (t + 1) * kd].astype(F32)
        for h in range(HEADS):
            turned = block[:, h * rows : (h + 1) * rows, :].reshape(128, res).T
            bias_ref[h, :, t * 128 : (t + 1) * 128] = (
                turned + kb_ref[:, t * 128 : (t + 1) * 128]
            ) * LOG2E

    def end_col(c, carry):
        own = pl.ds(pl.multiple_of(c * rows, rows), rows)
        normed = layer_norm(zs_ref[:, own, :].reshape(res, ch), g2_ref[...])
        p = nn(normed, w2_ref[...])
        q = (p[:, :ch] * QSCALE).astype(BF16)
        k = p[:, ch : 2 * ch].astype(BF16)
        v = p[:, 2 * ch : 3 * ch].astype(BF16)
        gate = jax.nn.sigmoid(p[:, 3 * ch :] + gb2_ref[...])
        for s in range(res // tq):
            lo = s * tq
            o = attend(q[lo : lo + tq], k, v, bias_ref, lo, tq)
            gated = (o * gate[lo : lo + tq]).astype(BF16)
            span = slice(lo // rows, (lo + tq) // rows)
            z2 = zs_ref[span, own, :].reshape(tq, ch) + nn(gated, ow2_ref[...])
            z2 = z2.astype(BF16).astype(F32)
            hid = nn(layer_norm(z2, g3_ref[...]), ti_ref[...]) + tb_ref[...]
            hid = jnp.maximum(hid, 0.0).astype(BF16)
            z3 = z2 + nn(hid, to_ref[...])
            zs_ref[span, own, :] = z3.reshape(tq // rows, rows, ch)
        return carry

    lax.fori_loop(0, rows, end_col, 0)
    send_z[...] = zs_ref[...].astype(BF16)

    @pl.loop(1, n)
    def _(t):
        p = peer_of(t)
        share(4, send_z.at[p], recv_o, p).start()

    recv_o[me] = send_z[me]

    @pl.loop(1, n)
    def _(t):
        p = peer_of(t)
        arrived(4, send_z.at[p], recv_o, p).wait()

    zs_ref[...] = recv_o[...].astype(F32)

    def out_row(r, carry):
        out_ref[r] = zs_ref[:, pl.ds(r, rows, stride=rows), :].reshape(res, ch).astype(BF16)
        return carry

    lax.fori_loop(0, rows, out_row, 0)


def solution(mesh):
    nx, ny = mesh.shape["gx"], mesh.shape["gy"]
    n = nx * ny

    def local(x, mask, g1, w1, gb1, bw1, ow1, g2, w2, gb2, bw2, ow2, g3, ti, tb, to):
        rows, res, ch = x.shape
        tq = min(res, 256)
        vmem = pl.BlockSpec(memory_space=pltpu.VMEM)
        row = lambda t: t.reshape(1, -1)
        return pl.pallas_call(
            functools.partial(kernel, nx, ny, tq),
            out_shape=jax.ShapeDtypeStruct(x.shape, x.dtype),
            in_specs=[vmem, pl.BlockSpec(memory_space=pltpu.SMEM)] + [vmem] * 14,
            out_specs=vmem,
            scratch_shapes=[
                pltpu.VMEM((rows, res, ch), BF16),
                pltpu.VMEM((rows, res, ch), BF16),
                pltpu.VMEM((rows, res, ch), BF16),
                pltpu.VMEM((rows, res, ch), BF16),
                pltpu.VMEM((HEADS, res, res), F32),
                pltpu.VMEM((1, res), F32),
                pltpu.VMEM((n, rows * rows, ch), F32),
                pltpu.VMEM((8, 128), F32),
                pltpu.VMEM((n, 8, 128), F32),
                pltpu.VMEM((HEADS * rows, res), BF16),
                pltpu.VMEM((n, HEADS * rows, res), BF16),
                pltpu.VMEM((HEADS * rows, res), BF16),
                pltpu.VMEM((n, HEADS * rows, res), BF16),
                pltpu.VMEM((n, rows * rows, ch), BF16),
                pltpu.VMEM((n, rows * rows, ch), BF16),
                pltpu.VMEM((n, rows * rows, ch), BF16),
                pltpu.SemaphoreType.DMA((5, n)),
                pltpu.SemaphoreType.DMA((5, n)),
            ],
            compiler_params=pltpu.CompilerParams(
                collective_id=0, has_side_effects=True, vmem_limit_bytes=66 * 1000 * 1000
            ),
        )(
            x, mask, row(g1), w1, row(gb1), bw1, ow1, row(g2), w2, row(gb2), bw2, ow2,
            row(g3), ti, row(tb), to,
        )

    placed = (P(("gx", "gy"), None, None), P(("gx", "gy"))) + (P(),) * 14
    return jax.shard_map(
        local, mesh=mesh, in_specs=placed, out_specs=P(("gx", "gy"), None, None), check_vma=False
    )
```

```python
import functools
import math

import jax
import jax.numpy as jnp
from jax import lax
from jax.experimental import pallas as pl
from jax.experimental.pallas import tpu as pltpu
from jax.sharding import PartitionSpec as P

HEADS = 4
HEAD_DIM = 32
BIG = 1000000000.0
LOG2E = math.log2(math.e)
QSCALE = HEAD_DIM ** (-0.5) * LOG2E
MESH = pl.DeviceIdType.MESH
F32 = jnp.float32
BF16 = jnp.bfloat16


def nn(a, b):
    return lax.dot_general(a, b, (((1,), (0,)), ((), ())), preferred_element_type=F32)


def nt(a, b):
    return lax.dot_general(a, b, (((1,), (1,)), ((), ())), preferred_element_type=F32)


def layer_norm(x, gain):
    mean = jnp.mean(x, axis=-1, keepdims=True)
    cent = x - mean
    var = jnp.mean(cent * cent, axis=-1, keepdims=True)
    return (cent * lax.rsqrt(var + 1e-05) * gain).astype(BF16)


def bias_rows(w, r, rows, normed):
    shape = (HEADS * rows, HEADS)
    place = lax.broadcasted_iota(jnp.int32, shape, 0) == (
        lax.broadcasted_iota(jnp.int32, shape, 1) * rows + r
    )
    spread = nn(place.astype(F32).astype(BF16), w).astype(BF16)
    return nt(spread, normed)


def head_mask(shape, h):
    lane = lax.broadcasted_iota(jnp.int32, shape, 1)
    return (lane >= h * HEAD_DIM) & (lane < (h + 1) * HEAD_DIM)


def attend(q, k, v, bias_ref, start, size):
    channels = q.shape[1]
    total = None
    for h in range(HEADS):
        mask = head_mask(k.shape, h)
        zero = jnp.zeros_like(k)
        scores = nt(q, jnp.where(mask, k, zero)) + bias_ref[h, pl.ds(start, size), :]
        top = jnp.max(scores, axis=-1, keepdims=True)
        weights = jnp.exp2(scores - top).astype(BF16)
        side = jnp.concatenate(
            [jnp.where(mask, v, zero), jnp.where(mask, jnp.ones_like(v), zero)], axis=1
        )
        part = nn(weights, side)
        total = part if total is None else total + part
    return total[:, :channels] / total[:, channels:]


def kernel(
    nx,
    ny,
    tq,
    x_ref,
    mask_ref,
    g1_ref,
    w1_ref,
    gb1_ref,
    bw1_ref,
    ow1_ref,
    g2_ref,
    w2_ref,
    gb2_ref,
    bw2_ref,
    ow2_ref,
    g3_ref,
    ti_ref,
    tb_ref,
    to_ref,
    out_ref,
    a_ref,
    q_ref,
    k_ref,
    v_ref,
    bias_ref,
    kb_ref,
    zs_ref,
    send_m,
    recv_m,
    recv_a,
    recv_b,
    send_z,
    recv_z,
    recv_o,
    ssem,
    rsem,
    fsem,
    lsem,
):
    n = nx * ny
    rows, res, ch = x_ref.shape
    me = lax.axis_index("gx") * ny + lax.axis_index("gy")

    def peer_of(t):
        return lax.rem(me + t, n)

    def coords(p):
        return (p // ny, lax.rem(p, ny))

    barrier = pltpu.get_barrier_semaphore()

    @pl.loop(1, n)
    def _(t):
        pl.semaphore_signal(barrier, inc=1, device_id=coords(peer_of(t)), device_id_type=MESH)

    def move(kind, src, dst, p, slot):
        return pltpu.make_async_remote_copy(
            src_ref=src,
            dst_ref=dst,
            send_sem=ssem.at[kind, slot],
            recv_sem=rsem.at[kind, slot],
            device_id=coords(p),
            device_id_type=MESH,
        )

    def share(kind, src, dst, p):
        return pltpu.make_async_remote_copy(
            src_ref=src,
            dst_ref=dst,
            send_sem=ssem.at[kind, p],
            recv_sem=rsem.at[kind, me],
            device_id=coords(p),
            device_id_type=MESH,
        )

    gx, gy = lax.axis_index("gx"), lax.axis_index("gy")
    core = lax.rem(gx, 2)
    half = nx // 2
    partner = (gx + 1 - 2 * core) * ny + gy

    def line_peer(t):
        return gx * ny + lax.rem(gy + t, ny)

    def plane_peer(t):
        return (lax.rem(gx // 2 + t, half) * 2 + core) * ny + gy

    def relay(kind, buf, t, s):
        @pl.loop(1, half)
        def _(u):
            q = plane_peer(u)
            pltpu.make_async_remote_copy(
                src_ref=buf.at[s],
                dst_ref=buf.at[s],
                send_sem=fsem.at[kind, t, u],
                recv_sem=rsem.at[kind, s],
                device_id=coords(q),
                device_id_type=MESH,
            ).start()

        hand(kind, buf, s).start()

    def hand(kind, buf, s):
        return move(kind, buf.at[s], buf.at[s], partner, s)

    def gather_start(kind, buf):
        @pl.loop(1, ny)
        def _(t):
            p = line_peer(t)
            pltpu.make_async_remote_copy(
                src_ref=buf.at[me],
                dst_ref=buf.at[me],
                send_sem=lsem.at[kind, t],
                recv_sem=rsem.at[kind, me],
                device_id=coords(p),
                device_id_type=MESH,
            ).start()

        relay(kind, buf, 0, me)

    def gather_finish(kind, buf):
        @pl.loop(1, ny)
        def _(t):
            p = line_peer(t)
            move(kind, buf.at[p], buf.at[p], p, p).wait_recv()
            relay(kind, buf, t, p)

        @pl.loop(0, ny)
        def _(t):
            @pl.loop(1, half)
            def _(u):
                s = plane_peer(u) - gy + lax.rem(gy + t, ny)
                move(kind, buf.at[s], buf.at[s], partner, s).wait_recv()
                hand(kind, buf, s).start()

        @pl.loop(0, ny)
        def _(t):
            @pl.loop(0, half)
            def _(u):
                s = plane_peer(u) - gy + lax.rem(gy + t, ny)
                o = s + (1 - 2 * core) * ny
                move(kind, buf.at[o], buf.at[o], partner, o).wait_recv()
                hand(kind, buf, s).wait_send()

            @pl.loop(1, half)
            def _(u):
                pltpu.make_async_remote_copy(
                    src_ref=buf.at[me],
                    dst_ref=buf.at[me],
                    send_sem=fsem.at[kind, t, u],
                    recv_sem=rsem.at[kind, me],
                    device_id=coords(partner),
                    device_id_type=MESH,
                ).wait_send()

        @pl.loop(1, ny)
        def _(t):
            pltpu.make_async_remote_copy(
                src_ref=buf.at[me],
                dst_ref=buf.at[me],
                send_sem=lsem.at[kind, t],
                recv_sem=rsem.at[kind, me],
                device_id=coords(partner),
                device_id_type=MESH,
            ).wait_send()

    def spread_pair(kind, src, dst, g):
        part = pl.ds(pl.multiple_of(g * 2 * rows, 2 * rows), 2 * rows)

        @pl.loop(1, n)
        def _(t):
            p = peer_of(t)
            share(kind, src.at[p, part], dst.at[me, part], p).start()

        dst[me, part] = src[me, part]

    def spread_finish(kind, src, dst):
        @pl.loop(1, n)
        def _(t):
            p = peer_of(t)
            move(kind, src.at[p], dst.at[p], p, p).wait()

    def norm_row(r, acc):
        normed = layer_norm(x_ref[r].astype(F32), g1_ref[...])
        a_ref[r] = normed
        return acc + bias_rows(bw1_ref[...], r, rows, normed)

    acc = lax.fori_loop(0, rows, norm_row, jnp.zeros((HEADS * rows, res), F32))
    recv_a[me] = acc.astype(BF16)
    lane = lax.broadcasted_iota(jnp.int32, (1, 128), 1)
    vec = jnp.zeros((1, 128), F32)
    for t in range(rows):
        vec = jnp.where(lane == lax.rem(me * rows, 128) + t, mask_ref[t].astype(F32), vec)
    send_m[...] = vec

    pl.semaphore_wait(barrier, n - 1)

    gather_start(0, recv_a)

    @pl.loop(1, n)
    def _(t):
        p = peer_of(t)
        share(2, send_m, recv_m.at[me], p).start()

    recv_m[me] = send_m[...]

    def project_row(r, carry):
        p = nn(a_ref[r], w1_ref[:, : 3 * ch])
        q_ref[r] = (p[:, :ch] * QSCALE).astype(BF16)
        k_ref[r] = p[:, ch : 2 * ch].astype(BF16)
        v_ref[r] = p[:, 2 * ch :].astype(BF16)
        return carry

    lax.fori_loop(0, rows, project_row, 0)

    gather_finish(0, recv_a)

    @pl.loop(1, n)
    def _(t):
        p = peer_of(t)
        move(2, send_m, recv_m.at[p], p, p).wait()

    kd = 128 // rows
    key_mask = jnp.concatenate(
        [jnp.sum(recv_m[t * kd : (t + 1) * kd], axis=0) for t in range(res // 128)], axis=1
    )
    kb_ref[...] = (key_mask - 1.0) * BIG

    def start_bias(d, carry):
        block = (recv_a[d].astype(F32) + kb_ref[...]) * LOG2E
        for h in range(HEADS):
            bias_ref[h, pl.ds(pl.multiple_of(d * rows, rows), rows), :] = block[
                h * rows : (h + 1) * rows
            ]
        return carry

    lax.fori_loop(0, n, start_bias, 0)

    def start_pair(g, acc):
        found = []
        for c in range(res // tq):
            lo = c * tq
            blocks, rise = [], None
            for e in range(2):
                r = 2 * g + e
                o = attend(q_ref[r, lo : lo + tq, :], k_ref[r], v_ref[r], bias_ref, lo, tq)
                gl = nn(a_ref[r, lo : lo + tq, :], w1_ref[:, 3 * ch :])
                gated = (o * jax.nn.sigmoid(gl + gb1_ref[...])).astype(BF16)
                z1 = x_ref[r, lo : lo + tq, :].astype(F32) + nn(gated, ow1_ref[...])
                z1 = z1.astype(BF16).astype(F32)
                blocks.append(z1.reshape(tq // rows, rows, ch))
                part = bias_rows(bw2_ref[...], r, rows, layer_norm(z1, g2_ref[...]))
                rise = part if rise is None else rise + part
            send_z[
                lo // rows : (lo + tq) // rows,
                pl.ds(pl.multiple_of(g * 2 * rows, 2 * rows), 2 * rows),
                :,
            ] = jnp.concatenate(blocks, axis=1).astype(BF16)
            found.append(rise)
        spread_pair(3, send_z, recv_z, g)
        return acc + (found[0] if len(found) == 1 else jnp.concatenate(found, axis=1))

    acc = lax.fori_loop(0, rows // 2, start_pair, jnp.zeros((HEADS * rows, res), F32))
    recv_b[me] = acc.astype(BF16)
    gather_start(1, recv_b)
    gather_finish(1, recv_b)
    spread_finish(3, send_z, recv_z)

    zs_ref[...] = recv_z[...].astype(F32)
    for t in range(res // 128):
        block = recv_b[t * kd : (t + 1) * kd].astype(F32)
        for h in range(HEADS):
            turned = block[:, h * rows : (h + 1) * rows, :].reshape(128, res).T
            bias_ref[h, :, t * 128 : (t + 1) * 128] = (
                turned + kb_ref[:, t * 128 : (t + 1) * 128]
            ) * LOG2E

    def end_pair(g, carry):
        ready = []
        for e in range(2):
            z1 = zs_ref[:, pl.ds(2 * g + e, rows, stride=rows), :].reshape(res, ch)
            p = nn(layer_norm(z1, g2_ref[...]), w2_ref[...])
            q = (p[:, :ch] * QSCALE).astype(BF16)
            k = p[:, ch : 2 * ch].astype(BF16)
            v = p[:, 2 * ch : 3 * ch].astype(BF16)
            gate = jax.nn.sigmoid(p[:, 3 * ch :] + gb2_ref[...])
            ready.append((z1, q, k, v, gate))
        for s in range(res // tq):
            lo = s * tq
            blocks = []
            for z1, q, k, v, gate in ready:
                o = attend(q[lo : lo + tq], k, v, bias_ref, lo, tq)
                gated = (o * gate[lo : lo + tq]).astype(BF16)
                z2 = z1[lo : lo + tq] + nn(gated, ow2_ref[...])
                z2 = z2.astype(BF16).astype(F32)
                hid = nn(layer_norm(z2, g3_ref[...]), ti_ref[...]) + tb_ref[...]
                hid = jnp.maximum(hid, 0.0).astype(BF16)
                z3 = z2 + nn(hid, to_ref[...])
                blocks.append(z3.reshape(tq // rows, rows, ch))
            send_z[
                lo // rows : (lo + tq) // rows,
                pl.ds(pl.multiple_of(g * 2 * rows, 2 * rows), 2 * rows),
                :,
            ] = jnp.concatenate(blocks, axis=1).astype(BF16)
        spread_pair(4, send_z, recv_o, g)
        return carry

    lax.fori_loop(0, rows // 2, end_pair, 0)
    spread_finish(4, send_z, recv_o)

    zs_ref[...] = recv_o[...].astype(F32)

    def out_row(r, carry):
        out_ref[r] = zs_ref[:, pl.ds(r, rows, stride=rows), :].reshape(res, ch).astype(BF16)
        return carry

    lax.fori_loop(0, rows, out_row, 0)


def solution(mesh):
    nx, ny = mesh.shape["gx"], mesh.shape["gy"]
    n = nx * ny

    def local(x, mask, g1, w1, gb1, bw1, ow1, g2, w2, gb2, bw2, ow2, g3, ti, tb, to):
        rows, res, ch = x.shape
        tq = 256 if res <= 256 else 128
        vmem = pl.BlockSpec(memory_space=pltpu.VMEM)
        row = lambda t: t.reshape(1, -1)
        return pl.pallas_call(
            functools.partial(kernel, nx, ny, tq),
            out_shape=jax.ShapeDtypeStruct(x.shape, x.dtype),
            in_specs=[vmem, pl.BlockSpec(memory_space=pltpu.SMEM)] + [vmem] * 14,
            out_specs=vmem,
            scratch_shapes=[
                pltpu.VMEM((rows, res, ch), BF16),
                pltpu.VMEM((rows, res, ch), BF16),
                pltpu.VMEM((rows, res, ch), BF16),
                pltpu.VMEM((rows, res, ch), BF16),
                pltpu.VMEM((HEADS, res, res), F32),
                pltpu.VMEM((1, res), F32),
                pltpu.VMEM((n, rows * rows, ch), F32),
                pltpu.VMEM((1, 128), F32),
                pltpu.VMEM((n, 1, 128), F32),
                pltpu.VMEM((n, HEADS * rows, res), BF16),
                pltpu.VMEM((n, HEADS * rows, res), BF16),
                pltpu.VMEM((n, rows * rows, ch), BF16),
                pltpu.VMEM((n, rows * rows, ch), BF16),
                pltpu.VMEM((n, rows * rows, ch), BF16),
                pltpu.SemaphoreType.DMA((5, n)),
                pltpu.SemaphoreType.DMA((5, n)),
                pltpu.SemaphoreType.DMA((2, ny, nx // 2)),
                pltpu.SemaphoreType.DMA((2, ny)),
            ],
            compiler_params=pltpu.CompilerParams(
                collective_id=0, has_side_effects=True, vmem_limit_bytes=66 * 1000 * 1000
            ),
        )(
            x, mask, row(g1), w1, row(gb1), bw1.T, ow1, row(g2), w2, row(gb2), bw2.T, ow2,
            row(g3), ti, row(tb), to,
        )

    placed = (P(("gx", "gy"), None, None), P(("gx", "gy"))) + (P(),) * 14
    return jax.shard_map(
        local, mesh=mesh, in_specs=placed, out_specs=P(("gx", "gy"), None, None), check_vma=False
    )
```

```python
import functools
import math

import jax
import jax.numpy as jnp
from jax import lax
from jax.experimental import pallas as pl
from jax.experimental.pallas import tpu as pltpu
from jax.sharding import PartitionSpec as P

HEADS = 4
HEAD_DIM = 32
BIG = 1000000000.0
LOG2E = math.log2(math.e)
QSCALE = HEAD_DIM ** (-0.5) * LOG2E
MESH = pl.DeviceIdType.MESH
F32 = jnp.float32
BF16 = jnp.bfloat16


def nn(a, b):
    return lax.dot_general(a, b, (((1,), (0,)), ((), ())), preferred_element_type=F32)


def nt(a, b):
    return lax.dot_general(a, b, (((1,), (1,)), ((), ())), preferred_element_type=F32)


def layer_norm(x, gain):
    mean = jnp.mean(x, axis=-1, keepdims=True)
    cent = x - mean
    var = jnp.mean(cent * cent, axis=-1, keepdims=True)
    return (cent * lax.rsqrt(var + 1e-05) * gain).astype(BF16)


def bias_rows(w, r, rows, normed):
    shape = (HEADS * rows, HEADS)
    place = lax.broadcasted_iota(jnp.int32, shape, 0) == (
        lax.broadcasted_iota(jnp.int32, shape, 1) * rows + r
    )
    spread = nn(place.astype(F32).astype(BF16), w).astype(BF16)
    return nt(spread, normed)


def head_mask(shape, h):
    lane = lax.broadcasted_iota(jnp.int32, shape, 1)
    return (lane >= h * HEAD_DIM) & (lane < (h + 1) * HEAD_DIM)


def attend(q, k, v, bias_ref, start, size):
    channels = q.shape[1]
    total = None
    for h in range(HEADS):
        mask = head_mask(k.shape, h)
        zero = jnp.zeros_like(k)
        scores = nt(q, jnp.where(mask, k, zero)) + bias_ref[h, pl.ds(start, size), :]
        top = jnp.max(scores, axis=-1, keepdims=True)
        weights = jnp.exp2(scores - top).astype(BF16)
        side = jnp.concatenate(
            [jnp.where(mask, v, zero), jnp.where(mask, jnp.ones_like(v), zero)], axis=1
        )
        part = nn(weights, side)
        total = part if total is None else total + part
    return total[:, :channels] / total[:, channels:]


def kernel(
    nx,
    ny,
    tq,
    x_ref,
    mask_ref,
    g1_ref,
    w1_ref,
    gb1_ref,
    bw1_ref,
    ow1_ref,
    g2_ref,
    w2_ref,
    gb2_ref,
    bw2_ref,
    ow2_ref,
    g3_ref,
    ti_ref,
    tb_ref,
    to_ref,
    out_ref,
    a_ref,
    q_ref,
    k_ref,
    v_ref,
    bias_ref,
    kb_ref,
    zs_ref,
    send_m,
    recv_m,
    recv_a,
    recv_b,
    send_z,
    recv_z,
    recv_o,
    ssem,
    rsem,
    fsem,
    lsem,
):
    n = nx * ny
    rows, res, ch = x_ref.shape
    me = lax.axis_index("gx") * ny + lax.axis_index("gy")

    def peer_of(t):
        return lax.rem(me + t, n)

    def coords(p):
        return (p // ny, lax.rem(p, ny))

    barrier = pltpu.get_barrier_semaphore()

    @pl.loop(1, n)
    def _(t):
        pl.semaphore_signal(barrier, inc=1, device_id=coords(peer_of(t)), device_id_type=MESH)

    def move(kind, src, dst, p, slot):
        return pltpu.make_async_remote_copy(
            src_ref=src,
            dst_ref=dst,
            send_sem=ssem.at[kind, slot],
            recv_sem=rsem.at[kind, slot],
            device_id=coords(p),
            device_id_type=MESH,
        )

    def share(kind, src, dst, p):
        return pltpu.make_async_remote_copy(
            src_ref=src,
            dst_ref=dst,
            send_sem=ssem.at[kind, p],
            recv_sem=rsem.at[kind, me],
            device_id=coords(p),
            device_id_type=MESH,
        )

    gx, gy = lax.axis_index("gx"), lax.axis_index("gy")
    core = lax.rem(gx, 2)
    half = nx // 2
    partner = (gx + 1 - 2 * core) * ny + gy

    def line_peer(t):
        return gx * ny + lax.rem(gy + t, ny)

    def plane_peer(t):
        return (lax.rem(gx // 2 + t, half) * 2 + core) * ny + gy

    def relay(kind, buf, t, s):
        @pl.loop(1, half)
        def _(u):
            q = plane_peer(u)
            pltpu.make_async_remote_copy(
                src_ref=buf.at[s],
                dst_ref=buf.at[s],
                send_sem=fsem.at[kind, t, u],
                recv_sem=rsem.at[kind, s],
                device_id=coords(q),
                device_id_type=MESH,
            ).start()

        hand(kind, buf, s).start()

    def hand(kind, buf, s):
        return move(kind, buf.at[s], buf.at[s], partner, s)

    def gather_start(kind, buf):
        @pl.loop(1, ny)
        def _(t):
            p = line_peer(t)
            pltpu.make_async_remote_copy(
                src_ref=buf.at[me],
                dst_ref=buf.at[me],
                send_sem=lsem.at[kind, t],
                recv_sem=rsem.at[kind, me],
                device_id=coords(p),
                device_id_type=MESH,
            ).start()

        relay(kind, buf, 0, me)

    def gather_finish(kind, buf):
        @pl.loop(1, ny)
        def _(t):
            p = line_peer(t)
            move(kind, buf.at[p], buf.at[p], p, p).wait_recv()
            relay(kind, buf, t, p)

        @pl.loop(0, ny)
        def _(t):
            @pl.loop(1, half)
            def _(u):
                s = plane_peer(u) - gy + lax.rem(gy + t, ny)
                move(kind, buf.at[s], buf.at[s], partner, s).wait_recv()
                hand(kind, buf, s).start()

        @pl.loop(0, ny)
        def _(t):
            @pl.loop(0, half)
            def _(u):
                s = plane_peer(u) - gy + lax.rem(gy + t, ny)
                o = s + (1 - 2 * core) * ny
                move(kind, buf.at[o], buf.at[o], partner, o).wait_recv()
                hand(kind, buf, s).wait_send()

            @pl.loop(1, half)
            def _(u):
                pltpu.make_async_remote_copy(
                    src_ref=buf.at[me],
                    dst_ref=buf.at[me],
                    send_sem=fsem.at[kind, t, u],
                    recv_sem=rsem.at[kind, me],
                    device_id=coords(partner),
                    device_id_type=MESH,
                ).wait_send()

        @pl.loop(1, ny)
        def _(t):
            pltpu.make_async_remote_copy(
                src_ref=buf.at[me],
                dst_ref=buf.at[me],
                send_sem=lsem.at[kind, t],
                recv_sem=rsem.at[kind, me],
                device_id=coords(partner),
                device_id_type=MESH,
            ).wait_send()

    def spread_pair(kind, src, dst, g):
        part = pl.ds(pl.multiple_of(g * 2 * rows, 2 * rows), 2 * rows)

        @pl.loop(1, n)
        def _(t):
            p = peer_of(t)
            share(kind, src.at[p, part], dst.at[me, part], p).start()

        dst[me, part] = src[me, part]

    def spread_finish(kind, src, dst):
        @pl.loop(1, n)
        def _(t):
            p = peer_of(t)
            move(kind, src.at[p], dst.at[p], p, p).wait()

    def norm_row(r, acc):
        normed = layer_norm(x_ref[r].astype(F32), g1_ref[...])
        a_ref[r] = normed
        return acc + bias_rows(bw1_ref[...], r, rows, normed)

    acc = lax.fori_loop(0, rows, norm_row, jnp.zeros((HEADS * rows, res), F32))
    recv_a[me] = acc.astype(BF16)
    lane = lax.broadcasted_iota(jnp.int32, (1, 128), 1)
    vec = jnp.zeros((1, 128), F32)
    for t in range(rows):
        vec = jnp.where(lane == lax.rem(me * rows, 128) + t, mask_ref[t].astype(F32), vec)
    send_m[...] = vec

    pl.semaphore_wait(barrier, n - 1)

    gather_start(0, recv_a)

    @pl.loop(1, n)
    def _(t):
        p = peer_of(t)
        share(2, send_m, recv_m.at[me], p).start()

    recv_m[me] = send_m[...]

    def project_row(r, carry):
        p = nn(a_ref[r], w1_ref[:, : 3 * ch])
        q_ref[r] = (p[:, :ch] * QSCALE).astype(BF16)
        k_ref[r] = p[:, ch : 2 * ch].astype(BF16)
        v_ref[r] = p[:, 2 * ch :].astype(BF16)
        return carry

    lax.fori_loop(0, rows, project_row, 0)

    gather_finish(0, recv_a)

    @pl.loop(1, n)
    def _(t):
        p = peer_of(t)
        move(2, send_m, recv_m.at[p], p, p).wait()

    kd = 128 // rows
    key_mask = jnp.concatenate(
        [jnp.sum(recv_m[t * kd : (t + 1) * kd], axis=0) for t in range(res // 128)], axis=1
    )
    kb_ref[...] = (key_mask - 1.0) * BIG

    def start_bias(d, carry):
        block = (recv_a[d].astype(F32) + kb_ref[...]) * LOG2E
        for h in range(HEADS):
            bias_ref[h, pl.ds(pl.multiple_of(d * rows, rows), rows), :] = block[
                h * rows : (h + 1) * rows
            ]
        return carry

    lax.fori_loop(0, n, start_bias, 0)

    early = rows // 4

    def start_pair(g, acc):
        found = []
        for c in range(res // tq):
            lo = c * tq
            blocks, rise = [], None
            for e in range(2):
                r = 2 * g + e
                o = attend(q_ref[r, lo : lo + tq, :], k_ref[r], v_ref[r], bias_ref, lo, tq)
                gl = nn(a_ref[r, lo : lo + tq, :], w1_ref[:, 3 * ch :])
                gated = (o * jax.nn.sigmoid(gl + gb1_ref[...])).astype(BF16)
                z1 = x_ref[r, lo : lo + tq, :].astype(F32) + nn(gated, ow1_ref[...])
                z1 = z1.astype(BF16).astype(F32)
                blocks.append(z1.reshape(tq // rows, rows, ch))
                part = bias_rows(bw2_ref[...], r, rows, layer_norm(z1, g2_ref[...]))
                rise = part if rise is None else rise + part
            send_z[
                lo // rows : (lo + tq) // rows,
                pl.ds(pl.multiple_of(g * 2 * rows, 2 * rows), 2 * rows),
                :,
            ] = jnp.concatenate(blocks, axis=1).astype(BF16)
            found.append(rise)

        @pl.when(g < early)
        def _():
            spread_pair(3, send_z, recv_z, g)

        return acc + (found[0] if len(found) == 1 else jnp.concatenate(found, axis=1))

    acc = lax.fori_loop(0, rows // 2, start_pair, jnp.zeros((HEADS * rows, res), F32))
    recv_b[me] = acc.astype(BF16)
    gather_start(1, recv_b)

    @pl.loop(early, rows // 2)
    def _(g):
        spread_pair(3, send_z, recv_z, g)

    gather_finish(1, recv_b)
    spread_finish(3, send_z, recv_z)

    zs_ref[...] = recv_z[...].astype(F32)
    for t in range(res // 128):
        block = recv_b[t * kd : (t + 1) * kd].astype(F32)
        for h in range(HEADS):
            turned = block[:, h * rows : (h + 1) * rows, :].reshape(128, res).T
            bias_ref[h, :, t * 128 : (t + 1) * 128] = (
                turned + kb_ref[:, t * 128 : (t + 1) * 128]
            ) * LOG2E

    def end_pair(g, carry):
        ready = []
        for e in range(2):
            z1 = zs_ref[:, pl.ds(2 * g + e, rows, stride=rows), :].reshape(res, ch)
            p = nn(layer_norm(z1, g2_ref[...]), w2_ref[...])
            q = (p[:, :ch] * QSCALE).astype(BF16)
            k = p[:, ch : 2 * ch].astype(BF16)
            v = p[:, 2 * ch : 3 * ch].astype(BF16)
            gate = jax.nn.sigmoid(p[:, 3 * ch :] + gb2_ref[...])
            ready.append((z1, q, k, v, gate))
        for s in range(res // tq):
            lo = s * tq
            blocks = []
            for z1, q, k, v, gate in ready:
                o = attend(q[lo : lo + tq], k, v, bias_ref, lo, tq)
                gated = (o * gate[lo : lo + tq]).astype(BF16)
                z2 = z1[lo : lo + tq] + nn(gated, ow2_ref[...])
                z2 = z2.astype(BF16).astype(F32)
                hid = nn(layer_norm(z2, g3_ref[...]), ti_ref[...]) + tb_ref[...]
                hid = jnp.maximum(hid, 0.0).astype(BF16)
                z3 = z2 + nn(hid, to_ref[...])
                blocks.append(z3.reshape(tq // rows, rows, ch))
            send_z[
                lo // rows : (lo + tq) // rows,
                pl.ds(pl.multiple_of(g * 2 * rows, 2 * rows), 2 * rows),
                :,
            ] = jnp.concatenate(blocks, axis=1).astype(BF16)
        spread_pair(4, send_z, recv_o, g)
        return carry

    lax.fori_loop(0, rows // 2, end_pair, 0)
    spread_finish(4, send_z, recv_o)

    zs_ref[...] = recv_o[...].astype(F32)

    def out_row(r, carry):
        out_ref[r] = zs_ref[:, pl.ds(r, rows, stride=rows), :].reshape(res, ch).astype(BF16)
        return carry

    lax.fori_loop(0, rows, out_row, 0)


def solution(mesh):
    nx, ny = mesh.shape["gx"], mesh.shape["gy"]
    n = nx * ny

    def local(x, mask, g1, w1, gb1, bw1, ow1, g2, w2, gb2, bw2, ow2, g3, ti, tb, to):
        rows, res, ch = x.shape
        tq = 256 if res <= 256 else 128
        vmem = pl.BlockSpec(memory_space=pltpu.VMEM)
        row = lambda t: t.reshape(1, -1)
        return pl.pallas_call(
            functools.partial(kernel, nx, ny, tq),
            out_shape=jax.ShapeDtypeStruct(x.shape, x.dtype),
            in_specs=[vmem, pl.BlockSpec(memory_space=pltpu.SMEM)] + [vmem] * 14,
            out_specs=vmem,
            scratch_shapes=[
                pltpu.VMEM((rows, res, ch), BF16),
                pltpu.VMEM((rows, res, ch), BF16),
                pltpu.VMEM((rows, res, ch), BF16),
                pltpu.VMEM((rows, res, ch), BF16),
                pltpu.VMEM((HEADS, res, res), F32),
                pltpu.VMEM((1, res), F32),
                pltpu.VMEM((n, rows * rows, ch), F32),
                pltpu.VMEM((1, 128), F32),
                pltpu.VMEM((n, 1, 128), F32),
                pltpu.VMEM((n, HEADS * rows, res), BF16),
                pltpu.VMEM((n, HEADS * rows, res), BF16),
                pltpu.VMEM((n, rows * rows, ch), BF16),
                pltpu.VMEM((n, rows * rows, ch), BF16),
                pltpu.VMEM((n, rows * rows, ch), BF16),
                pltpu.SemaphoreType.DMA((5, n)),
                pltpu.SemaphoreType.DMA((5, n)),
                pltpu.SemaphoreType.DMA((2, ny, nx // 2)),
                pltpu.SemaphoreType.DMA((2, ny)),
            ],
            compiler_params=pltpu.CompilerParams(
                collective_id=0, has_side_effects=True, vmem_limit_bytes=66 * 1000 * 1000
            ),
        )(
            x, mask, row(g1), w1, row(gb1), bw1.T, ow1, row(g2), w2, row(gb2), bw2.T, ow2,
            row(g3), ti, row(tb), to,
        )

    placed = (P(("gx", "gy"), None, None), P(("gx", "gy"))) + (P(),) * 14
    return jax.shard_map(
        local, mesh=mesh, in_specs=placed, out_specs=P(("gx", "gy"), None, None), check_vma=False
    )
```

```python
import functools
import math

import jax
import jax.numpy as jnp
from jax import lax
from jax.experimental import pallas as pl
from jax.experimental.pallas import tpu as pltpu
from jax.sharding import PartitionSpec as P

HEADS = 4
HEAD_DIM = 32
BIG = 1000000000.0
LOG2E = math.log2(math.e)
QSCALE = HEAD_DIM ** (-0.5) * LOG2E
MESH = pl.DeviceIdType.MESH
F32 = jnp.float32
BF16 = jnp.bfloat16


def nn(a, b):
    return lax.dot_general(a, b, (((1,), (0,)), ((), ())), preferred_element_type=F32)


def nt(a, b):
    return lax.dot_general(a, b, (((1,), (1,)), ((), ())), preferred_element_type=F32)


def layer_norm(x, gain):
    mean = jnp.mean(x, axis=-1, keepdims=True)
    cent = x - mean
    var = jnp.mean(cent * cent, axis=-1, keepdims=True)
    return (cent * lax.rsqrt(var + 1e-05) * gain).astype(BF16)


def bias_rows(w, r, rows, normed):
    shape = (HEADS * rows, HEADS)
    place = lax.broadcasted_iota(jnp.int32, shape, 0) == (
        lax.broadcasted_iota(jnp.int32, shape, 1) * rows + r
    )
    spread = nn(place.astype(F32).astype(BF16), w).astype(BF16)
    return nt(spread, normed)


def head_mask(shape, h):
    lane = lax.broadcasted_iota(jnp.int32, shape, 1)
    return (lane >= h * HEAD_DIM) & (lane < (h + 1) * HEAD_DIM)


def attend(q, k, v, bias_ref, start, size):
    channels = q.shape[1]
    total = None
    for h in range(HEADS):
        mask = head_mask(k.shape, h)
        zero = jnp.zeros_like(k)
        scores = nt(q, jnp.where(mask, k, zero)) + bias_ref[h, pl.ds(start, size), :]
        top = jnp.max(scores, axis=-1, keepdims=True)
        weights = jnp.exp2(scores - top).astype(BF16)
        side = jnp.concatenate(
            [jnp.where(mask, v, zero), jnp.where(mask, jnp.ones_like(v), zero)], axis=1
        )
        part = nn(weights, side)
        total = part if total is None else total + part
    return total[:, :channels] / total[:, channels:]


def kernel(
    nx,
    ny,
    tq,
    x_ref,
    mask_ref,
    g1_ref,
    w1_ref,
    gb1_ref,
    bw1_ref,
    ow1_ref,
    g2_ref,
    w2_ref,
    gb2_ref,
    bw2_ref,
    ow2_ref,
    g3_ref,
    ti_ref,
    tb_ref,
    to_ref,
    out_ref,
    q_ref,
    k_ref,
    v_ref,
    bias_ref,
    kb_ref,
    zs_ref,
    recv_a,
    recv_b,
    send_z,
    recv_z,
    recv_o,
    ssem,
    rsem,
    fsem,
    lsem,
):
    n = nx * ny
    rows, res, ch = x_ref.shape
    me = lax.axis_index("gx") * ny + lax.axis_index("gy")

    def peer_of(t):
        return lax.rem(me + t, n)

    def coords(p):
        return (p // ny, lax.rem(p, ny))


    def move(kind, src, dst, p, slot):
        return pltpu.make_async_remote_copy(
            src_ref=src,
            dst_ref=dst,
            send_sem=ssem.at[kind, slot],
            recv_sem=rsem.at[kind, slot],
            device_id=coords(p),
            device_id_type=MESH,
        )

    def share(kind, src, dst, p):
        return pltpu.make_async_remote_copy(
            src_ref=src,
            dst_ref=dst,
            send_sem=ssem.at[kind, p],
            recv_sem=rsem.at[kind, me],
            device_id=coords(p),
            device_id_type=MESH,
        )

    gx, gy = lax.axis_index("gx"), lax.axis_index("gy")
    a_ref = out_ref
    core = lax.rem(gx, 2)
    half = nx // 2
    partner = (gx + 1 - 2 * core) * ny + gy

    def line_peer(t):
        return gx * ny + lax.rem(gy + t, ny)

    def plane_peer(t):
        return (lax.rem(gx // 2 + t, half) * 2 + core) * ny + gy

    barrier = pltpu.get_barrier_semaphore()

    def greet(p):
        pl.semaphore_signal(barrier, inc=1, device_id=coords(p), device_id_type=MESH)

    for t in range(1, ny):
        greet(line_peer(t))
    for t in range(1, half):
        greet(plane_peer(t))
    greet(partner)

    def relay(kind, buf, t, s):
        @pl.loop(1, half)
        def _(u):
            q = plane_peer(u)
            pltpu.make_async_remote_copy(
                src_ref=buf.at[s],
                dst_ref=buf.at[s],
                send_sem=fsem.at[kind, t, u],
                recv_sem=rsem.at[kind, s],
                device_id=coords(q),
                device_id_type=MESH,
            ).start()

        hand(kind, buf, s).start()

    def hand(kind, buf, s):
        return move(kind, buf.at[s], buf.at[s], partner, s)

    def gather_start(kind, buf):
        @pl.loop(1, ny)
        def _(t):
            p = line_peer(t)
            pltpu.make_async_remote_copy(
                src_ref=buf.at[me],
                dst_ref=buf.at[me],
                send_sem=lsem.at[kind, t],
                recv_sem=rsem.at[kind, me],
                device_id=coords(p),
                device_id_type=MESH,
            ).start()

        relay(kind, buf, 0, me)

    def gather_finish(kind, buf):
        @pl.loop(1, ny)
        def _(t):
            p = line_peer(t)
            move(kind, buf.at[p], buf.at[p], p, p).wait_recv()
            relay(kind, buf, t, p)

        @pl.loop(0, ny)
        def _(t):
            @pl.loop(1, half)
            def _(u):
                s = plane_peer(u) - gy + lax.rem(gy + t, ny)
                move(kind, buf.at[s], buf.at[s], partner, s).wait_recv()
                hand(kind, buf, s).start()

        @pl.loop(0, ny)
        def _(t):
            @pl.loop(0, half)
            def _(u):
                s = plane_peer(u) - gy + lax.rem(gy + t, ny)
                o = s + (1 - 2 * core) * ny
                move(kind, buf.at[o], buf.at[o], partner, o).wait_recv()
                hand(kind, buf, s).wait_send()

            @pl.loop(1, half)
            def _(u):
                pltpu.make_async_remote_copy(
                    src_ref=buf.at[me],
                    dst_ref=buf.at[me],
                    send_sem=fsem.at[kind, t, u],
                    recv_sem=rsem.at[kind, me],
                    device_id=coords(partner),
                    device_id_type=MESH,
                ).wait_send()

        @pl.loop(1, ny)
        def _(t):
            pltpu.make_async_remote_copy(
                src_ref=buf.at[me],
                dst_ref=buf.at[me],
                send_sem=lsem.at[kind, t],
                recv_sem=rsem.at[kind, me],
                device_id=coords(partner),
                device_id_type=MESH,
            ).wait_send()

    def spread_pair(kind, src, dst, g):
        part = pl.ds(pl.multiple_of(g * 2 * rows, 2 * rows), 2 * rows)

        @pl.loop(1, n)
        def _(t):
            p = peer_of(t)
            share(kind, src.at[p, part], dst.at[me, part], p).start()

        dst[me, part] = src[me, part]

    def spread_finish(kind, src, dst):
        @pl.loop(1, n)
        def _(t):
            p = peer_of(t)
            move(kind, src.at[p], dst.at[p], p, p).wait()

    def norm_row(r, acc):
        normed = layer_norm(x_ref[r].astype(F32), g1_ref[...])
        a_ref[r] = normed
        return acc + bias_rows(bw1_ref[...], r, rows, normed)

    acc = lax.fori_loop(0, rows, norm_row, jnp.zeros((HEADS * rows, res), F32))
    deep, wide = HEADS * rows, res // 128
    for t in range(wide):
        recv_a[me, t * deep : (t + 1) * deep, :] = acc[:, t * 128 : (t + 1) * 128].astype(BF16)
    lane = lax.broadcasted_iota(jnp.int32, (16, 128), 1)
    vec = jnp.zeros((16, 128), F32)
    for t in range(rows):
        vec = jnp.where(lane == lax.rem(me * rows, 128) + t, mask_ref[t].astype(F32), vec)
    recv_a[me, wide * deep :, :] = vec.astype(BF16)

    pl.semaphore_wait(barrier, ny + half - 1)

    gather_start(0, recv_a)

    def project_row(r, carry):
        p = nn(a_ref[r], w1_ref[:, : 3 * ch])
        q_ref[r] = (p[:, :ch] * QSCALE).astype(BF16)
        k_ref[r] = p[:, ch : 2 * ch].astype(BF16)
        v_ref[r] = p[:, 2 * ch :].astype(BF16)
        return carry

    lax.fori_loop(0, rows, project_row, 0)

    gather_finish(0, recv_a)

    kd = 128 // rows
    masks = [
        jnp.sum(recv_a[t * kd : (t + 1) * kd, wide * deep :, :].astype(F32), axis=0)[:1]
        for t in range(wide)
    ]
    key_mask = masks[0] if wide == 1 else jnp.concatenate(masks, axis=1)
    kb_ref[...] = (key_mask - 1.0) * BIG

    def start_bias(d, carry):
        for t in range(wide):
            span = slice(t * 128, (t + 1) * 128)
            block = recv_a[d, t * deep : (t + 1) * deep, :].astype(F32)
            block = (block + kb_ref[:, span]) * LOG2E
            for h in range(HEADS):
                bias_ref[h, pl.ds(pl.multiple_of(d * rows, rows), rows), span] = block[
                    h * rows : (h + 1) * rows
                ]
        return carry

    lax.fori_loop(0, n, start_bias, 0)

    early = rows // 4

    def start_pair(g, acc):
        found = []
        for c in range(res // tq):
            lo = c * tq
            blocks, rise = [], None
            for e in range(2):
                r = 2 * g + e
                o = attend(q_ref[r, lo : lo + tq, :], k_ref[r], v_ref[r], bias_ref, lo, tq)
                gl = nn(a_ref[r, lo : lo + tq, :], w1_ref[:, 3 * ch :])
                gated = (o * jax.nn.sigmoid(gl + gb1_ref[...])).astype(BF16)
                z1 = x_ref[r, lo : lo + tq, :].astype(F32) + nn(gated, ow1_ref[...])
                z1 = z1.astype(BF16).astype(F32)
                blocks.append(z1.reshape(tq // rows, rows, ch))
                part = bias_rows(bw2_ref[...], r, rows, layer_norm(z1, g2_ref[...]))
                rise = part if rise is None else rise + part
            send_z[
                lo // rows : (lo + tq) // rows,
                pl.ds(pl.multiple_of(g * 2 * rows, 2 * rows), 2 * rows),
                :,
            ] = jnp.concatenate(blocks, axis=1).astype(BF16)
            found.append(rise)

        @pl.when(g < early)
        def _():
            spread_pair(3, send_z, recv_z, g)

        return acc + (found[0] if len(found) == 1 else jnp.concatenate(found, axis=1))

    acc = lax.fori_loop(0, rows // 2, start_pair, jnp.zeros((HEADS * rows, res), F32))
    recv_b[me] = acc.astype(BF16)
    gather_start(1, recv_b)

    @pl.loop(early, rows // 2)
    def _(g):
        spread_pair(3, send_z, recv_z, g)

    gather_finish(1, recv_b)
    spread_finish(3, send_z, recv_z)

    zs_ref[...] = recv_z[...].astype(F32)
    for t in range(res // 128):
        block = recv_b[t * kd : (t + 1) * kd].astype(F32)
        for h in range(HEADS):
            turned = block[:, h * rows : (h + 1) * rows, :].reshape(128, res).T
            bias_ref[h, :, t * 128 : (t + 1) * 128] = (
                turned + kb_ref[:, t * 128 : (t + 1) * 128]
            ) * LOG2E

    def end_pair(g, carry):
        ready = []
        for e in range(2):
            z1 = zs_ref[:, pl.ds(2 * g + e, rows, stride=rows), :].reshape(res, ch)
            p = nn(layer_norm(z1, g2_ref[...]), w2_ref[...])
            q = (p[:, :ch] * QSCALE).astype(BF16)
            k = p[:, ch : 2 * ch].astype(BF16)
            v = p[:, 2 * ch : 3 * ch].astype(BF16)
            gate = jax.nn.sigmoid(p[:, 3 * ch :] + gb2_ref[...])
            ready.append((z1, q, k, v, gate))
        for s in range(res // tq):
            lo = s * tq
            blocks = []
            for z1, q, k, v, gate in ready:
                o = attend(q[lo : lo + tq], k, v, bias_ref, lo, tq)
                gated = (o * gate[lo : lo + tq]).astype(BF16)
                z2 = z1[lo : lo + tq] + nn(gated, ow2_ref[...])
                z2 = z2.astype(BF16).astype(F32)
                hid = nn(layer_norm(z2, g3_ref[...]), ti_ref[...]) + tb_ref[...]
                hid = jnp.maximum(hid, 0.0).astype(BF16)
                z3 = z2 + nn(hid, to_ref[...])
                blocks.append(z3.reshape(tq // rows, rows, ch))
            send_z[
                lo // rows : (lo + tq) // rows,
                pl.ds(pl.multiple_of(g * 2 * rows, 2 * rows), 2 * rows),
                :,
            ] = jnp.concatenate(blocks, axis=1).astype(BF16)
        spread_pair(4, send_z, recv_o, g)
        return carry

    lax.fori_loop(0, rows // 2, end_pair, 0)
    spread_finish(4, send_z, recv_o)

    zs_ref[...] = recv_o[...].astype(F32)

    def out_row(r, carry):
        out_ref[r] = zs_ref[:, pl.ds(r, rows, stride=rows), :].reshape(res, ch).astype(BF16)
        return carry

    lax.fori_loop(0, rows, out_row, 0)


def solution(mesh):
    nx, ny = mesh.shape["gx"], mesh.shape["gy"]
    n = nx * ny

    def local(x, mask, g1, w1, gb1, bw1, ow1, g2, w2, gb2, bw2, ow2, g3, ti, tb, to):
        rows, res, ch = x.shape
        tq = 256 if res <= 256 else 128
        vmem = pl.BlockSpec(memory_space=pltpu.VMEM)
        row = lambda t: t.reshape(1, -1)
        return pl.pallas_call(
            functools.partial(kernel, nx, ny, tq),
            out_shape=jax.ShapeDtypeStruct(x.shape, x.dtype),
            in_specs=[vmem, pl.BlockSpec(memory_space=pltpu.SMEM)] + [vmem] * 14,
            out_specs=vmem,
            scratch_shapes=[
                pltpu.VMEM((rows, res, ch), BF16),
                pltpu.VMEM((rows, res, ch), BF16),
                pltpu.VMEM((rows, res, ch), BF16),
                pltpu.VMEM((HEADS, res, res), F32),
                pltpu.VMEM((1, res), F32),
                pltpu.VMEM((n, rows * rows, ch), F32),
                pltpu.VMEM((n, HEADS * rows * (res // 128) + 16, 128), BF16),
                pltpu.VMEM((n, HEADS * rows, res), BF16),
                pltpu.VMEM((n, rows * rows, ch), BF16),
                pltpu.VMEM((n, rows * rows, ch), BF16),
                pltpu.VMEM((n, rows * rows, ch), BF16),
                pltpu.SemaphoreType.DMA((5, n)),
                pltpu.SemaphoreType.DMA((5, n)),
                pltpu.SemaphoreType.DMA((2, ny, nx // 2)),
                pltpu.SemaphoreType.DMA((2, ny)),
            ],
            compiler_params=pltpu.CompilerParams(
                collective_id=0, has_side_effects=True, vmem_limit_bytes=66 * 1000 * 1000
            ),
        )(
            x, mask, row(g1), w1, row(gb1), bw1.T, ow1, row(g2), w2, row(gb2), bw2.T, ow2,
            row(g3), ti, row(tb), to,
        )

    placed = (P(("gx", "gy"), None, None), P(("gx", "gy"))) + (P(),) * 14
    return jax.shard_map(
        local, mesh=mesh, in_specs=placed, out_specs=P(("gx", "gy"), None, None), check_vma=False
    )
```

```python
import functools
import math

import jax
import jax.numpy as jnp
from jax import lax
from jax.experimental import pallas as pl
from jax.experimental.pallas import tpu as pltpu
from jax.sharding import PartitionSpec as P

HEADS = 4
HEAD_DIM = 32
BIG = 1000000000.0
LOG2E = math.log2(math.e)
QSCALE = HEAD_DIM ** (-0.5) * LOG2E
MESH = pl.DeviceIdType.MESH
F32 = jnp.float32
BF16 = jnp.bfloat16


def nn(a, b):
    return lax.dot_general(a, b, (((1,), (0,)), ((), ())), preferred_element_type=F32)


def nt(a, b):
    return lax.dot_general(a, b, (((1,), (1,)), ((), ())), preferred_element_type=F32)


def layer_norm(x, gain):
    mean = jnp.mean(x, axis=-1, keepdims=True)
    cent = x - mean
    var = jnp.mean(cent * cent, axis=-1, keepdims=True)
    return (cent * lax.rsqrt(var + 1e-05) * gain).astype(BF16)


def bias_rows(w, r, rows, normed):
    shape = (HEADS * rows, HEADS)
    place = lax.broadcasted_iota(jnp.int32, shape, 0) == (
        lax.broadcasted_iota(jnp.int32, shape, 1) * rows + r
    )
    spread = nn(place.astype(F32).astype(BF16), w).astype(BF16)
    return nt(spread, normed)


def head_mask(shape, h):
    lane = lax.broadcasted_iota(jnp.int32, shape, 1)
    return (lane >= h * HEAD_DIM) & (lane < (h + 1) * HEAD_DIM)


def attend(q, k, v, bias_ref, start, size):
    channels = q.shape[1]
    total = None
    for h in range(HEADS):
        mask = head_mask(k.shape, h)
        zero = jnp.zeros_like(k)
        scores = nt(q, jnp.where(mask, k, zero)) + bias_ref[h, pl.ds(start, size), :]
        top = jnp.max(scores, axis=-1, keepdims=True)
        weights = jnp.exp2(scores - top).astype(BF16)
        side = jnp.concatenate(
            [jnp.where(mask, v, zero), jnp.where(mask, jnp.ones_like(v), zero)], axis=1
        )
        part = nn(weights, side)
        total = part if total is None else total + part
    return total[:, :channels] / total[:, channels:]


def kernel(
    nx,
    ny,
    tq,
    x_ref,
    mask_ref,
    g1_ref,
    w1_ref,
    gb1_ref,
    bw1_ref,
    ow1_ref,
    g2_ref,
    w2_ref,
    gb2_ref,
    bw2_ref,
    ow2_ref,
    g3_ref,
    ti_ref,
    tb_ref,
    to_ref,
    out_ref,
    q_ref,
    k_ref,
    v_ref,
    bias_ref,
    kb_ref,
    zs_ref,
    recv_a,
    recv_b,
    send_z,
    recv_z,
    recv_o,
    ssem,
    rsem,
    fsem,
    lsem,
):
    n = nx * ny
    rows, res, ch = x_ref.shape
    me = lax.axis_index("gx") * ny + lax.axis_index("gy")

    def peer_of(t):
        return lax.rem(me + t, n)

    def coords(p):
        return (p // ny, lax.rem(p, ny))


    def move(kind, src, dst, p, slot):
        return pltpu.make_async_remote_copy(
            src_ref=src,
            dst_ref=dst,
            send_sem=ssem.at[kind, slot],
            recv_sem=rsem.at[kind, slot],
            device_id=coords(p),
            device_id_type=MESH,
        )

    def share(kind, src, dst, p):
        return pltpu.make_async_remote_copy(
            src_ref=src,
            dst_ref=dst,
            send_sem=ssem.at[kind, p],
            recv_sem=rsem.at[kind, me],
            device_id=coords(p),
            device_id_type=MESH,
        )

    gx, gy = lax.axis_index("gx"), lax.axis_index("gy")
    a_ref = out_ref
    core = lax.rem(gx, 2)
    half = nx // 2
    partner = (gx + 1 - 2 * core) * ny + gy

    def line_peer(t):
        return gx * ny + lax.rem(gy + t, ny)

    def plane_peer(t):
        return (lax.rem(gx // 2 + t, half) * 2 + core) * ny + gy

    barrier = pltpu.get_barrier_semaphore()

    def greet(p):
        pl.semaphore_signal(barrier, inc=1, device_id=coords(p), device_id_type=MESH)

    for t in range(1, ny):
        greet(line_peer(t))
    for t in range(1, half):
        greet(plane_peer(t))
    greet(partner)

    def relay(kind, buf, t, s):
        @pl.loop(1, half)
        def _(u):
            q = plane_peer(u)
            pltpu.make_async_remote_copy(
                src_ref=buf.at[s],
                dst_ref=buf.at[s],
                send_sem=fsem.at[kind, t, u],
                recv_sem=rsem.at[kind, s],
                device_id=coords(q),
                device_id_type=MESH,
            ).start()

        hand(kind, buf, s).start()

    def hand(kind, buf, s):
        return move(kind, buf.at[s], buf.at[s], partner, s)

    def gather_start(kind, buf):
        @pl.loop(1, ny)
        def _(t):
            p = line_peer(t)
            pltpu.make_async_remote_copy(
                src_ref=buf.at[me],
                dst_ref=buf.at[me],
                send_sem=lsem.at[kind, t],
                recv_sem=rsem.at[kind, me],
                device_id=coords(p),
                device_id_type=MESH,
            ).start()

        relay(kind, buf, 0, me)

    def gather_finish(kind, buf):
        @pl.loop(1, ny)
        def _(t):
            p = line_peer(t)
            move(kind, buf.at[p], buf.at[p], p, p).wait_recv()
            relay(kind, buf, t, p)

        @pl.loop(0, ny)
        def _(t):
            @pl.loop(1, half)
            def _(u):
                s = plane_peer(u) - gy + lax.rem(gy + t, ny)
                move(kind, buf.at[s], buf.at[s], partner, s).wait_recv()
                hand(kind, buf, s).start()

        @pl.loop(0, ny)
        def _(t):
            @pl.loop(0, half)
            def _(u):
                s = plane_peer(u) - gy + lax.rem(gy + t, ny)
                o = s + (1 - 2 * core) * ny
                move(kind, buf.at[o], buf.at[o], partner, o).wait_recv()
                hand(kind, buf, s).wait_send()

            @pl.loop(1, half)
            def _(u):
                pltpu.make_async_remote_copy(
                    src_ref=buf.at[me],
                    dst_ref=buf.at[me],
                    send_sem=fsem.at[kind, t, u],
                    recv_sem=rsem.at[kind, me],
                    device_id=coords(partner),
                    device_id_type=MESH,
                ).wait_send()

        @pl.loop(1, ny)
        def _(t):
            pltpu.make_async_remote_copy(
                src_ref=buf.at[me],
                dst_ref=buf.at[me],
                send_sem=lsem.at[kind, t],
                recv_sem=rsem.at[kind, me],
                device_id=coords(partner),
                device_id_type=MESH,
            ).wait_send()

    def spread_pair(kind, src, dst, g):
        part = pl.ds(pl.multiple_of(g * 2 * rows, 2 * rows), 2 * rows)

        @pl.loop(1, n)
        def _(t):
            p = peer_of(t)
            share(kind, src.at[p, part], dst.at[me, part], p).start()

        dst[me, part] = src[me, part]

    def spread_finish(kind, src, dst):
        @pl.loop(1, n)
        def _(t):
            p = peer_of(t)
            move(kind, src.at[p], dst.at[p], p, p).wait()

    def norm_row(r, acc):
        normed = layer_norm(x_ref[r].astype(F32), g1_ref[...])
        a_ref[r] = normed
        return acc + bias_rows(bw1_ref[...], r, rows, normed)

    acc = lax.fori_loop(0, rows, norm_row, jnp.zeros((HEADS * rows, res), F32))
    deep, wide = HEADS * rows, res // 128
    for t in range(wide):
        recv_a[me, t * deep : (t + 1) * deep, :] = acc[:, t * 128 : (t + 1) * 128].astype(BF16)
    lane = lax.broadcasted_iota(jnp.int32, (16, 128), 1)
    vec = jnp.zeros((16, 128), F32)
    for t in range(rows):
        vec = jnp.where(lane == lax.rem(me * rows, 128) + t, mask_ref[t].astype(F32), vec)
    recv_a[me, wide * deep :, :] = vec.astype(BF16)

    pl.semaphore_wait(barrier, ny + half - 1)

    gather_start(0, recv_a)

    def project_row(r, carry):
        p = nn(a_ref[r], w1_ref[:, : 3 * ch])
        q_ref[r] = (p[:, :ch] * QSCALE).astype(BF16)
        k_ref[r] = p[:, ch : 2 * ch].astype(BF16)
        v_ref[r] = p[:, 2 * ch :].astype(BF16)
        return carry

    lax.fori_loop(0, rows, project_row, 0)

    gather_finish(0, recv_a)

    kd = 128 // rows
    masks = [
        jnp.sum(recv_a[t * kd : (t + 1) * kd, wide * deep :, :].astype(F32), axis=0)[:1]
        for t in range(wide)
    ]
    key_mask = masks[0] if wide == 1 else jnp.concatenate(masks, axis=1)
    kb_ref[...] = (key_mask - 1.0) * BIG

    def start_bias(d, carry):
        for t in range(wide):
            span = slice(t * 128, (t + 1) * 128)
            block = recv_a[d, t * deep : (t + 1) * deep, :].astype(F32)
            block = (block + kb_ref[:, span]) * LOG2E
            for h in range(HEADS):
                bias_ref[h, pl.ds(pl.multiple_of(d * rows, rows), rows), span] = block[
                    h * rows : (h + 1) * rows
                ]
        return carry

    lax.fori_loop(0, n, start_bias, 0)

    early = rows // 4

    def start_pair(g, acc):
        found = []
        for c in range(res // tq):
            lo = c * tq
            blocks, rise = [], None
            for e in range(2):
                r = 2 * g + e
                o = attend(q_ref[r, lo : lo + tq, :], k_ref[r], v_ref[r], bias_ref, lo, tq)
                gl = nn(a_ref[r, lo : lo + tq, :], w1_ref[:, 3 * ch :])
                gated = (o * jax.nn.sigmoid(gl + gb1_ref[...])).astype(BF16)
                z1 = x_ref[r, lo : lo + tq, :].astype(F32) + nn(gated, ow1_ref[...])
                z1 = z1.astype(BF16).astype(F32)
                blocks.append(z1.reshape(tq // rows, rows, ch))
                part = bias_rows(bw2_ref[...], r, rows, layer_norm(z1, g2_ref[...]))
                rise = part if rise is None else rise + part
            send_z[
                lo // rows : (lo + tq) // rows,
                pl.ds(pl.multiple_of(g * 2 * rows, 2 * rows), 2 * rows),
                :,
            ] = jnp.concatenate(blocks, axis=1).astype(BF16)
            found.append(rise)

        @pl.when(g < early)
        def _():
            spread_pair(3, send_z, recv_z, g)

        return acc + (found[0] if len(found) == 1 else jnp.concatenate(found, axis=1))

    acc = lax.fori_loop(0, rows // 2, start_pair, jnp.zeros((HEADS * rows, res), F32))
    recv_b[me] = acc.astype(BF16)
    gather_start(1, recv_b)

    @pl.loop(early, rows // 2)
    def _(g):
        spread_pair(3, send_z, recv_z, g)

    gather_finish(1, recv_b)
    spread_finish(3, send_z, recv_z)

    zs_ref[...] = recv_z[...].astype(F32)
    for t in range(res // 128):
        block = recv_b[t * kd : (t + 1) * kd].astype(F32)
        for h in range(HEADS):
            turned = block[:, h * rows : (h + 1) * rows, :].reshape(128, res).T
            bias_ref[h, :, t * 128 : (t + 1) * 128] = (
                turned + kb_ref[:, t * 128 : (t + 1) * 128]
            ) * LOG2E

    te = min(tq, res // 2)

    def spread_some(g, first, last):
        part = pl.ds(pl.multiple_of(g * 2 * rows, 2 * rows), 2 * rows)

        @pl.loop(first, last)
        def _(p):
            @pl.when(p != me)
            def _():
                share(4, send_z.at[p, part], recv_o.at[me, part], p).start()

    def end_pair(g, carry):
        ready = []
        for e in range(2):
            z1 = zs_ref[:, pl.ds(2 * g + e, rows, stride=rows), :].reshape(res, ch)
            p = nn(layer_norm(z1, g2_ref[...]), w2_ref[...])
            q = (p[:, :ch] * QSCALE).astype(BF16)
            k = p[:, ch : 2 * ch].astype(BF16)
            v = p[:, 2 * ch : 3 * ch].astype(BF16)
            gate = jax.nn.sigmoid(p[:, 3 * ch :] + gb2_ref[...])
            ready.append((z1, q, k, v, gate))
        for s in range(res // te):
            lo = s * te
            blocks = []
            for z1, q, k, v, gate in ready:
                o = attend(q[lo : lo + te], k, v, bias_ref, lo, te)
                gated = (o * gate[lo : lo + te]).astype(BF16)
                z2 = z1[lo : lo + te] + nn(gated, ow2_ref[...])
                z2 = z2.astype(BF16).astype(F32)
                hid = nn(layer_norm(z2, g3_ref[...]), ti_ref[...]) + tb_ref[...]
                hid = jnp.maximum(hid, 0.0).astype(BF16)
                z3 = z2 + nn(hid, to_ref[...])
                blocks.append(z3.reshape(te // rows, rows, ch))
            send_z[
                lo // rows : (lo + te) // rows,
                pl.ds(pl.multiple_of(g * 2 * rows, 2 * rows), 2 * rows),
                :,
            ] = jnp.concatenate(blocks, axis=1).astype(BF16)
            spread_some(g, lo // rows, (lo + te) // rows)
        return carry

    lax.fori_loop(0, rows // 2, end_pair, 0)
    spread_finish(4, send_z, recv_o)
    recv_o[me] = send_z[me]

    zs_ref[...] = recv_o[...].astype(F32)

    def out_row(r, carry):
        out_ref[r] = zs_ref[:, pl.ds(r, rows, stride=rows), :].reshape(res, ch).astype(BF16)
        return carry

    lax.fori_loop(0, rows, out_row, 0)


def solution(mesh):
    nx, ny = mesh.shape["gx"], mesh.shape["gy"]
    n = nx * ny

    def local(x, mask, g1, w1, gb1, bw1, ow1, g2, w2, gb2, bw2, ow2, g3, ti, tb, to):
        rows, res, ch = x.shape
        tq = 256 if res <= 256 else 128
        vmem = pl.BlockSpec(memory_space=pltpu.VMEM)
        row = lambda t: t.reshape(1, -1)
        return pl.pallas_call(
            functools.partial(kernel, nx, ny, tq),
            out_shape=jax.ShapeDtypeStruct(x.shape, x.dtype),
            in_specs=[vmem, pl.BlockSpec(memory_space=pltpu.SMEM)] + [vmem] * 14,
            out_specs=vmem,
            scratch_shapes=[
                pltpu.VMEM((rows, res, ch), BF16),
                pltpu.VMEM((rows, res, ch), BF16),
                pltpu.VMEM((rows, res, ch), BF16),
                pltpu.VMEM((HEADS, res, res), F32),
                pltpu.VMEM((1, res), F32),
                pltpu.VMEM((n, rows * rows, ch), F32),
                pltpu.VMEM((n, HEADS * rows * (res // 128) + 16, 128), BF16),
                pltpu.VMEM((n, HEADS * rows, res), BF16),
                pltpu.VMEM((n, rows * rows, ch), BF16),
                pltpu.VMEM((n, rows * rows, ch), BF16),
                pltpu.VMEM((n, rows * rows, ch), BF16),
                pltpu.SemaphoreType.DMA((5, n)),
                pltpu.SemaphoreType.DMA((5, n)),
                pltpu.SemaphoreType.DMA((2, ny, nx // 2)),
                pltpu.SemaphoreType.DMA((2, ny)),
            ],
            compiler_params=pltpu.CompilerParams(
                collective_id=0, has_side_effects=True, vmem_limit_bytes=66 * 1000 * 1000
            ),
        )(
            x, mask, row(g1), w1, row(gb1), bw1.T, ow1, row(g2), w2, row(gb2), bw2.T, ow2,
            row(g3), ti, row(tb), to,
        )

    placed = (P(("gx", "gy"), None, None), P(("gx", "gy"))) + (P(),) * 14
    return jax.shard_map(
        local, mesh=mesh, in_specs=placed, out_specs=P(("gx", "gy"), None, None), check_vma=False
    )
```
